32 devices in a mesh: seq: 4 (over y, core), et: 8 (over z, x).
Axes of the slice: x: 2, y: 2, z: 4, core: 2. Of those that a mesh axis runs over, the one named last changes fastest.
Arguments:
- hidden_in: bfloat16 [128, 4096], P('seq'), may hold values from -6 to 6
- expert_ids: int32 [128, 2], P('seq'), may hold values from 0 to 7, all different within a row; in each aligned block of 32 rows (0 to 31, 32 to 63, ...) at most 10 rows name the same one
- gate_vals: bfloat16 [128, 2], P('seq'), may hold values from 0 to 1, as said below
- w_gate: bfloat16 [8, 4096, 14336], P('et', None, 'seq'), may hold values from -0.09375 to 0.09375
- w_up: bfloat16 [8, 4096, 14336], P('et', None, 'seq'), may hold values from -0.09375 to 0.09375
- w_down: bfloat16 [8, 14336, 4096], P('et', 'seq'), may hold values from -0.0625 to 0.0625
Outputs:
- mixed: bfloat16 [128, 4096], P('seq', 'et')
The draws below stay inside these ranges and needn't reach their ends.
Inputs may be any that keep to these rules, and one draw needn't show every extreme that they name: `expert_ids`: the rows of each token name different experts; within each block of 32 rows (the rows of one device) no expert is named by more than 10 rows. `gate_vals`: each token's two weights sum to 1 up to bfloat16 rounding, the first is not the smaller.
All inputs are finite; a program needn't handle non-finite values.
Results may differ from the reference program's by a relative error of at most 0.019.
Values may be sent and summed in bfloat16 or wider, within the bound.
A program may use at most 128 MiB of HBM per device.

```python
import math
import jax
import jax.numpy as jnp
import numpy as np
from jax import lax

D = 4096
FF = 14336
EXPERTS = 8
TOP = 2
TOK_DEV = 32
SLOTS = 10
GROUP = 1
TOKENS = 128
N_SEQ = 4


def draw_gate_vals(key, part):
    leading = jax.random.uniform(key, (TOKENS, 1), jnp.float32, 0.5, 0.9)
    return jnp.concatenate([leading, 1.0 - leading], axis=1).astype(jnp.bfloat16)


def spiked(drawn, stream_key, source, target, shards_of, factor):
    owner, partner = [(jnp.arange(drawn.shape[dim]) // (drawn.shape[dim] // shards_of)).reshape([-1 if axis == dim else 1 for axis in range(drawn.ndim)]) for dim in (source, target)]
    chosen = jax.random.permutation(stream_key, shards_of)[partner]
    strong = (owner == chosen) | (owner == (partner + shards_of // 2) % shards_of)
    return jnp.where(strong, factor * drawn, drawn)


def block_scale(key, extent, cuts, low, largest):
    gain = 1.0
    for position, shards_of in cuts:
        steps = jax.random.uniform(jax.random.fold_in(jax.random.fold_in(key, 6), position), (shards_of,), jnp.float32, low / len(cuts), largest / len(cuts))
        gain = gain * jnp.repeat(jnp.exp(steps), extent[position] // shards_of).reshape((-1,) + (1,) * (len(extent) - 1 - position))
    return gain


def shared_out(key, own, number, rows, number_of, top, most, slope):
    sequence = jax.random.permutation(key, number_of)
    crowded, usual = shares(number_of, rows * top, most, slope, True), shares(number_of, rows * top, most, slope, False)
    places = jnp.arange(number_of)

    def named(lengths, turn):
        used = int((lengths > 0).sum())
        fixed = max(1, used // 4)
        moved = fixed + (places - fixed + turn * (used - fixed)) % max(1, number_of - fixed)
        return jnp.zeros((number_of,), jnp.int32).at[sequence[jnp.where(places < fixed, places, moved)]].set(jnp.asarray(lengths, jnp.int32))

    lengths = jnp.where(number % 4 == 0, named(crowded, number // 4), named(usual, number - number // 4 - 1))
    mixed = jax.random.permutation(jax.random.fold_in(own, 3), number_of)
    source_of, receiver = mixed[0:number_of // 2 * 2:2], mixed[1:number_of // 2 * 2:2]
    margin = jnp.minimum(lengths[source_of] - 1, most - lengths[receiver]) // 2
    margin = jnp.where((source_of == sequence[0]) | (receiver == sequence[0]) | (lengths[receiver] == 0), 0, jnp.maximum(margin, 0))
    moved = jax.random.randint(jax.random.fold_in(own, 4), (number_of // 2,), 0, 1 << 20) % (margin + 1)
    lengths = lengths.at[source_of].add(-moved).at[receiver].add(moved)
    labels = jnp.searchsorted(jnp.cumsum(lengths), jnp.arange(rows * top), side="right").astype(jnp.int32)
    grid = labels.reshape(top, rows).T
    grid = grid[jax.random.permutation(jax.random.fold_in(own, 1), rows)]
    turn = jax.random.randint(jax.random.fold_in(own, 2), (rows, 1), 0, top)
    return jnp.take_along_axis(grid, (jnp.arange(top)[None, :] + turn) % top, axis=1)


def shares(count, total, reach, slope, full):
    weights = [(1 << 20) // math.isqrt(rank ** slope) + 1 for rank in range(1, count + 1)]
    largest = reach if full else min(reach, max(-(-total // count), total * weights[0] // sum(weights)))
    least = 1 if total - largest >= count - 1 else 0
    holding, rest = [largest] + [least] * (count - 1), total - largest - least * (count - 1)
    while rest > 0:
        free = [i for i in range(1, count) if holding[i] < largest] or [i for i in range(1, count) if holding[i] < reach]
        pool, remaining = sum([weights[i] for i in free]), rest
        for i in free:
            addition = min(reach - holding[i], max(1, remaining * weights[i] // pool), rest)
            holding[i] = holding[i] + addition
            rest = rest - addition
    return np.array(holding)


def scatter_about(own_key, shape, spread, bound, split=(), held_as=jnp.bfloat16):
    array = jax.random.normal(own_key, shape, jnp.float32) * spread
    if len(split) > 0:
        array = block_scale(own_key, shape, split, -0.22, 0.18) * array
    return jnp.clip(array, min=-bound, max=bound).astype(held_as)


def gaussian_with(key, dims, scale, reach, split, heavy, kind=jnp.bfloat16):
    array = scale * jax.random.normal(key, dims, jnp.float32)
    if split:
        array = array * block_scale(key, dims, split, -0.22, 0.18)
    return jnp.clip(spiked(array, jax.random.fold_in(key, 3), *heavy), -reach, reach).astype(kind)


def setup_inputs(seed: int = 0) -> dict:
    key_list = jax.random.split(jax.random.key(seed), 7)
    hidden_in = scatter_about(key_list[0], (TOKENS, D), 1.0, 6.0, ((0, 4),))
    expert_ids_keys = jax.random.split(jax.random.fold_in(key_list[1], 1), TOKENS // TOK_DEV)
    expert_ids_turns = jax.random.permutation(jax.random.fold_in(key_list[1], 3), TOKENS // TOK_DEV)
    expert_ids = jax.vmap(lambda own, number: shared_out(jax.random.fold_in(key_list[1], 2), own, number, TOK_DEV, EXPERTS, TOP, SLOTS, 2))(expert_ids_keys, expert_ids_turns).reshape((TOKENS, TOP))
    gate_vals = draw_gate_vals(jax.random.fold_in(key_list[6], 71), 0)
    w_gate = scatter_about(key_list[3], (EXPERTS * GROUP, D, FF // GROUP), D ** -0.5, 0.09375, ((0, 8), (2, 4)))
    w_up = scatter_about(key_list[4], (EXPERTS * GROUP, D, FF // GROUP), D ** -0.5, 0.09375, ((0, 8), (2, 4)))
    w_down = gaussian_with(key_list[5], (EXPERTS * GROUP, FF // GROUP, D), FF ** -0.5, 0.0625, ((0, 8), (1, 4)), (1, 2, 4, 2.0))
    return {"hidden_in": hidden_in, "expert_ids": expert_ids, "gate_vals": gate_vals, "w_gate": w_gate, "w_up": w_up, "w_down": w_down}


def slot_numbers(routed):
    flattened = routed.reshape(-1)
    one_hot = (flattened[:, None] == jnp.arange(EXPERTS, dtype=jnp.int32)[None, :]).astype(jnp.int32)
    earlier = jnp.cumsum(one_hot, axis=0) - one_hot
    return jnp.sum(earlier * one_hot, axis=1).reshape(routed.shape).astype(jnp.int32)


def reference(hidden_in, expert_ids, gate_vals, w_gate, w_up, w_down):
    group_size = w_gate.shape[0] // EXPERTS
    block_count = hidden_in.shape[0] // TOK_DEV
    run_width = FF // (group_size * N_SEQ)
    stream = hidden_in.reshape(block_count, TOK_DEV, D)
    routed = expert_ids.reshape(block_count, TOK_DEV, TOP)
    gates = gate_vals.astype(jnp.float32).reshape(block_count, TOK_DEV, TOP)
    slot_index = jax.vmap(slot_numbers)(routed)
    expert_range = jnp.arange(EXPERTS, dtype=jnp.int32)
    columns = jnp.arange(SLOTS, dtype=jnp.int32)
    matches = (routed[:, None, None, :, :] == expert_range[None, :, None, None, None]) & (slot_index[:, None, None, :, :] == columns[None, None, :, None, None])
    placing = jnp.sum(matches.astype(jnp.float32), axis=-1)
    combining = jnp.sum(jnp.where(matches, gates[:, None, None, :, :], 0.0), axis=-1)
    buffer = jnp.einsum("bect,btd->becd", placing, stream.astype(jnp.float32)).astype(jnp.bfloat16)
    row_count = block_count * SLOTS

    def run_expert(index):
        selected = buffer[:, index].reshape(row_count, D)
        gate_block = lax.dynamic_slice_in_dim(w_gate, index * group_size, group_size, 0)
        up_block = lax.dynamic_slice_in_dim(w_up, index * group_size, group_size, 0)
        down_block = lax.dynamic_slice_in_dim(w_down, index * group_size, group_size, 0)
        gate_full = jnp.transpose(gate_block, (1, 0, 2)).reshape(D, -1)
        up_full = jnp.transpose(up_block, (1, 0, 2)).reshape(D, -1)
        gate_part = jnp.dot(selected, gate_full, preferred_element_type=jnp.float32)
        up_part = jnp.dot(selected, up_full, preferred_element_type=jnp.float32)
        activations = (jax.nn.silu(gate_part) * up_part).astype(jnp.bfloat16)
        act_runs = jnp.transpose(activations.reshape(row_count, group_size, N_SEQ, run_width), (2, 0, 1, 3))
        down_runs = jnp.transpose(down_block.reshape(group_size, N_SEQ, run_width, D), (1, 0, 2, 3))

        def add_run(total, pair):
            act_run, down_run = pair
            piece = jnp.einsum("rgc,gcd->rgd", act_run.astype(jnp.float32), down_run.astype(jnp.float32), precision=lax.Precision.HIGHEST)
            rounded = lax.optimization_barrier(piece.astype(jnp.bfloat16))
            return total + rounded.astype(jnp.float32), None

        start = jnp.zeros((row_count, group_size, D), jnp.float32)
        total, unused = lax.scan(add_run, start, (act_runs, down_runs))
        return total

    expert_out = lax.map(run_expert, expert_range)
    expert_out = expert_out.reshape(EXPERTS, block_count, SLOTS, group_size, D)
    summed = jnp.einsum("bect,ebcgd->btd", combining, expert_out, precision=lax.Precision.HIGHEST)
    mixed = stream.astype(jnp.float32) + summed
    return mixed.reshape(block_count * TOK_DEV, D).astype(jnp.bfloat16)
```

```python
import functools

import jax
import jax.numpy as jnp
from jax import lax
from jax.experimental import pallas as pl
from jax.experimental.pallas import tpu as pltpu
from jax.sharding import PartitionSpec as P

EXPERTS = 8
SLOTS = 10
PAD = 16
WIDE = 512
DEPTH = 3
LAG = 3
MESH = pl.DeviceIdType.MESH


def slot_numbers(routed):
    flattened = routed.reshape(-1)
    one_hot = (flattened[:, None] == jnp.arange(EXPERTS, dtype=jnp.int32)[None, :]).astype(
        jnp.int32
    )
    earlier = jnp.cumsum(one_hot, axis=0) - one_hot
    return jnp.sum(earlier * one_hot, axis=1).reshape(routed.shape)


def local(hidden_in, expert_ids, gate_vals, w_gate, w_up, w_down):
    group_size = lax.axis_size("et") // EXPERTS
    expert_here = lax.axis_index("et") // group_size
    slot_index = slot_numbers(expert_ids)
    chosen = expert_ids == expert_here
    columns = jnp.arange(SLOTS, dtype=jnp.int32)
    matches = chosen[:, None, :] & (slot_index[:, None, :] == columns[None, :, None])
    placing = jnp.any(matches, axis=2).astype(jnp.bfloat16)
    combining = jnp.sum(jnp.where(matches, gate_vals.astype(jnp.float32)[:, None, :], 0.0), axis=2)
    buffer = jnp.dot(placing.T, hidden_in, preferred_element_type=jnp.float32).astype(jnp.bfloat16)
    gate_local = w_gate[0]
    up_local = w_up[0]
    down_local = w_down[0]
    segment = lax.all_gather(buffer, "seq", axis=0, tiled=True)
    gate_part = jnp.dot(segment, gate_local, preferred_element_type=jnp.float32)
    up_part = jnp.dot(segment, up_local, preferred_element_type=jnp.float32)
    activations = (jax.nn.silu(gate_part) * up_part).astype(jnp.bfloat16)
    partial_value = lax.psum_scatter(
        jnp.dot(activations, down_local, preferred_element_type=jnp.float32).astype(jnp.bfloat16),
        "seq",
        scatter_dimension=0,
        tiled=True,
    ).astype(jnp.float32)
    contribution = jnp.dot(combining, partial_value, precision=lax.Precision.HIGHEST)
    share_width = hidden_in.shape[1] // lax.axis_size("et")
    mixed_part = lax.psum_scatter(
        contribution.astype(jnp.bfloat16), "et", scatter_dimension=1, tiled=True
    ).astype(jnp.float32)
    residual_part = lax.dynamic_slice_in_dim(
        hidden_in, lax.axis_index("et") * share_width, share_width, 1
    )
    return (residual_part.astype(jnp.float32) + mixed_part).astype(jnp.bfloat16)


def kernel(
    n_et, n_wide,
    hidden, ids, gates, w_gate, w_up, w_down, out,
    xg, gu, dw, act, psend, precv, esend, erecv,
    gu_sem, d_sem, x_send, x_recv, p_send, p_recv, e_send, e_recv,
):
    seq, et = lax.axis_index("seq"), lax.axis_index("et")
    chip, core = seq // 2, seq % 2
    mate = chip * 2 + (1 - core)
    across = (1 - chip) * 2 + core
    corner = (1 - chip) * 2 + (1 - core)
    peers = (mate, across, corner)
    share = out.shape[1]
    half = hidden.shape[1] // 2
    tokens = hidden.shape[0]
    rows = 4 * PAD

    def pair(i):
        slot = i % DEPTH
        cols = pl.ds(pl.multiple_of(i * WIDE, WIDE), WIDE)
        return [
            pltpu.make_async_copy(w.at[0, :, cols], gu.at[k, slot], gu_sem.at[k, slot])
            for k, w in enumerate((w_gate, w_up))
        ]

    def target(i):
        return (et + 1 + i) % n_et

    def down(i):
        cols = pl.ds(pl.multiple_of(target(i) * share, share), share)
        return pltpu.make_async_copy(w_down.at[0, :, cols], dw.at[i], d_sem.at[i])

    def start_pair(i):
        for copy in pair(i):
            copy.start()

    for i in range(DEPTH):
        start_pair(i)
    down(0).start()
    down(1).start()

    barrier = pltpu.get_barrier_semaphore()
    for p in peers:
        pl.semaphore_signal(barrier, inc=1, device_id=(p, et), device_id_type=MESH)
    for i in range(n_et - 1):
        pl.semaphore_signal(barrier, inc=1, device_id=(seq, target(i)), device_id_type=MESH)

    first, second = ids[:, 0:1], ids[:, 1:2]
    earlier = (
        lax.broadcasted_iota(jnp.int32, (tokens, tokens), 1)
        < lax.broadcasted_iota(jnp.int32, (tokens, tokens), 0)
    ).astype(jnp.float32).astype(jnp.bfloat16)
    column = lax.broadcasted_iota(jnp.int32, (tokens, n_et * PAD), 1)

    def matched(expert, slot):
        named = ((first == expert) | (second == expert)).astype(jnp.float32)
        before = jnp.dot(earlier, named.astype(jnp.bfloat16), preferred_element_type=jnp.float32)
        return jnp.where(before == slot.astype(jnp.float32), named, 0.0)

    here = matched(jnp.full_like(column, 0) + et, column)
    placing = jnp.transpose(here)[:PAD, :].astype(jnp.bfloat16)
    xg[seq] = jnp.dot(placing, hidden[...], preferred_element_type=jnp.float32).astype(jnp.bfloat16)

    pl.semaphore_wait(barrier, len(peers) + n_et - 1)

    def move(block, cols, to, n):
        return pltpu.make_async_remote_copy(
            src_ref=xg.at[block, :, cols], dst_ref=xg.at[block, :, cols],
            send_sem=x_send.at[n], recv_sem=x_recv.at[n],
            device_id=(to, et), device_id_type=MESH,
        )

    halves = (pl.ds(0, half), pl.ds(half, half))
    far = [move(seq, halves[h], across, h) for h in range(2)]
    near = [move(seq, halves[h], mate, 2 + h) for h in range(2)]
    for copy in far + near:
        copy.start()
    relay = [move(across, halves[h], mate, 4 + h) for h in range(2)]
    for h in range(2):
        far[h].wait_recv()
        relay[h].start()
    for copy in near + relay:
        copy.wait_recv()

    def up_step(i, carry):
        slot = i % DEPTH
        for copy in pair(i):
            copy.wait()
        x = xg[...].reshape(rows, 2 * half)
        g = jnp.dot(x, gu[0, slot], preferred_element_type=jnp.float32)
        u = jnp.dot(x, gu[1, slot], preferred_element_type=jnp.float32)
        act[:, pl.ds(pl.multiple_of(i * WIDE, WIDE), WIDE)] = (
            g / (1.0 + jnp.exp(-g)) * u
        ).astype(jnp.bfloat16)

        @pl.when(i + DEPTH < n_wide)
        def _():
            start_pair(i + DEPTH)

        @pl.when((i >= 2) & (i < n_et))
        def _():
            down(i).start()

        return carry

    lax.fori_loop(0, n_wide, up_step, 0)
    for i in range(max(2, min(n_wide, n_et)), n_et):
        down(i).start()

    def scatter(i):
        return [
            pltpu.make_async_remote_copy(
                src_ref=psend.at[i, p], dst_ref=precv.at[i, r],
                send_sem=p_send.at[i, r], recv_sem=p_recv.at[i, r],
                device_id=(p, et), device_id_type=MESH,
            )
            for r, p in enumerate(peers)
        ]

    def give(i):
        return pltpu.make_async_remote_copy(
            src_ref=esend.at[i], dst_ref=erecv.at[i],
            send_sem=e_send.at[i], recv_sem=e_recv.at[i],
            device_id=(seq, target(i)), device_id_type=MESH,
        )

    def summed(i):
        for copy in scatter(i):
            copy.wait_recv()
        total = psend[i, seq].astype(jnp.float32)
        for r in range(len(peers)):
            total = total + precv[i, r].astype(jnp.float32)
        return total.astype(jnp.bfloat16)

    def pass_on(i):
        esend[i] = summed(i)
        give(i).start()

    def down_step(i, carry):
        down(i).wait()
        part = jnp.dot(act[...], dw[i], preferred_element_type=jnp.float32)
        psend[i] = part.astype(jnp.bfloat16).reshape(4, PAD, share)
        for copy in scatter(i):
            copy.start()

        @pl.when(i >= LAG)
        def _():
            pass_on(i - LAG)

        return carry

    lax.fori_loop(0, n_et, down_step, 0)
    for i in range(n_et - LAG, n_et - 1):
        pass_on(i)

    source = et + n_et - 1 - column // PAD
    source = jnp.where(source >= n_et, source - n_et, source)
    weight = jnp.where(
        first == source, gates[:, 0:1].astype(jnp.float32), gates[:, 1:2].astype(jnp.float32)
    )
    combining = (matched(source, column % PAD) * weight).astype(jnp.bfloat16)
    residual = hidden[:, pl.ds(pl.multiple_of(et * share, share), share)].astype(jnp.float32)

    erecv[n_et - 1] = summed(n_et - 1)
    for i in range(n_et - 1):
        give(i).wait_recv()
    mixed = jnp.dot(
        combining, erecv[...].reshape(n_et * PAD, share), preferred_element_type=jnp.float32
    )
    out[...] = (residual + mixed).astype(jnp.bfloat16)

    for copy in far + near + relay:
        copy.wait_send()
    for i in range(n_et):
        for copy in scatter(i):
            copy.wait_send()
    for i in range(n_et - 1):
        give(i).wait_send()


def fused(hidden_in, expert_ids, gate_vals, w_gate, w_up, w_down):
    n_et = lax.axis_size("et")
    tokens, width = hidden_in.shape
    units = w_gate.shape[2]
    share = width // n_et
    n_wide = units // WIDE
    vmem = pl.BlockSpec(memory_space=pltpu.VMEM)
    hbm = pl.BlockSpec(memory_space=pl.ANY)
    dma = pltpu.SemaphoreType.DMA
    return pl.pallas_call(
        functools.partial(kernel, n_et, n_wide),
        out_shape=jax.ShapeDtypeStruct((tokens, share), jnp.bfloat16),
        in_specs=[vmem] * 3 + [hbm] * 3,
        out_specs=vmem,
        scratch_shapes=[
            pltpu.VMEM((4, PAD, width), jnp.bfloat16),
            pltpu.VMEM((2, DEPTH, width, WIDE), jnp.bfloat16),
            pltpu.VMEM((n_et, units, share), jnp.bfloat16),
            pltpu.VMEM((4 * PAD, units), jnp.bfloat16),
            pltpu.VMEM((n_et, 4, PAD, share), jnp.bfloat16),
            pltpu.VMEM((n_et, 3, PAD, share), jnp.bfloat16),
            pltpu.VMEM((n_et, PAD, share), jnp.bfloat16),
            pltpu.VMEM((n_et, PAD, share), jnp.bfloat16),
            dma((2, DEPTH)),
            dma((n_et,)),
            dma((6,)),
            dma((6,)),
            dma((n_et, 3)),
            dma((n_et, 3)),
            dma((n_et,)),
            dma((n_et,)),
        ],
        compiler_params=pltpu.CompilerParams(
            collective_id=0, has_side_effects=True, vmem_limit_bytes=66_000_000
        ),
    )(hidden_in, expert_ids, gate_vals, w_gate, w_up, w_down)


def solution(mesh):
    in_specs = (
        P("seq", None),
        P("seq", None),
        P("seq", None),
        P("et", None, "seq"),
        P("et", None, "seq"),
        P("et", "seq", None),
    )
    out_specs = P("seq", "et")
    n_seq, n_et = mesh.shape["seq"], mesh.shape["et"]

    def layer(hidden_in, expert_ids, gate_vals, w_gate, w_up, w_down):
        width, units = w_gate.shape[1:]
        held = 2 * (2 * DEPTH * width * WIDE + units * width)
        fits = (
            n_seq == 4 and n_et == EXPERTS and units % WIDE == 0
            and units // WIDE > DEPTH and width % (n_et * 128) == 0 and held < 58_000_000
        )
        body = fused if fits else local
        return body(hidden_in, expert_ids, gate_vals, w_gate, w_up, w_down)

    return jax.shard_map(layer, mesh=mesh, in_specs=in_specs, out_specs=out_specs, check_vma=False)
```
